256 devices in a mesh: dp: 32 (over x_hi, z, core), tensor: 8 (over y, x_lo).
Axes of the slice: x: 4 (x_hi: 2, x_lo: 2; x = x_hi * 2 + x_lo), y: 4, z: 8, core: 2. Of those that a mesh axis runs over, the one named last changes fastest.
Arguments:
- grad_hidden: bfloat16 [4096, 14336], P('dp', 'tensor'), may hold values from -18 to 18
- gate: bfloat16 [4096, 14336], P('dp', 'tensor'), may hold values from -6 to 6
Outputs:
- factor: float32 [14336, 14336], P('tensor', 'dp')
The draws below stay inside these ranges and needn't reach their ends.
All inputs are finite; a program needn't handle non-finite values.
Results may differ from the reference program's by a relative error of at most 0.0065.
Values may be sent and summed in bfloat16 or wider, within the bound.
A program may use at most 128 MiB of HBM per device.

```python
import jax
import jax.numpy as jnp
from jax import lax

FF = 14336
TOKENS = 4096


def level_of(rng, extent, split, least, high):
    gain, own = 1.0, jax.random.fold_in(rng, 6)
    for dim, blocks in split:
        draws = jnp.exp(jax.random.uniform(jax.random.fold_in(own, dim), (blocks,), jnp.float32, least / len(split), high / len(split)))
        gain = gain * jnp.repeat(draws, extent[dim] // blocks).reshape([-1 if axis == dim else 1 for axis in range(len(extent))])
    return gain


def bell_draw(stream_key, dims, scale, most, shards=(), dtype=jnp.bfloat16):
    array = jax.random.normal(stream_key, dims, jnp.float32) * scale
    if len(shards) > 0:
        array = level_of(stream_key, dims, shards, -0.22, 0.18) * array
    return jnp.clip(array, min=-most, max=most).astype(dtype)


def setup_inputs(seed: int = 0) -> dict:
    splits = jax.random.split(jax.random.key(seed), 3)
    return {
        "grad_hidden": bell_draw(splits[0], (TOKENS, FF), 3.0, 18.0, ((0, 32), (1, 8))),
        "gate": bell_draw(splits[1], (TOKENS, FF), 1.0, 6.0, ((0, 32), (1, 8))),
    }


def reference(grad_hidden, gate):
    up_grad = (grad_hidden.astype(jnp.float32) * jax.nn.silu(gate.astype(jnp.float32))).astype(jnp.bfloat16)
    wide = up_grad.astype(jnp.float32)
    blocks = wide.reshape(wide.shape[0], FF // 1792 if FF % 1792 == 0 else 1, -1)
    blocks = jnp.transpose(blocks, (1, 0, 2))

    def column_block(piece):
        return jnp.dot(wide.T, piece, precision=lax.Precision.HIGHEST, preferred_element_type=jnp.float32)

    panels = lax.map(column_block, blocks)
    factor = jnp.transpose(panels, (1, 0, 2)).reshape(FF, FF)
    return factor / TOKENS
```

```python
import jax
import jax.numpy as jnp
from jax import lax
from jax.experimental import pallas as pl
from jax.experimental.pallas import tpu as pltpu
from jax.sharding import PartitionSpec as P

WIDTH = 1792
TOK = 128
UNITS = 16
PIECE = 112
COLS = 448
CUT = 896
A, B = 0, 1
SPAN = (pl.ds(0, CUT), pl.ds(CUT, WIDTH - CUT))
TILE = 256
NT = (((1,), (1,)), ((), ()))


def kernel(
    grad_ref, gate_ref, out_ref, rows, rows_o, cols, cols_o,
    row_recv, rowo_recv, spread_recv, piece_recv, colo_recv, ssem,
):
    dp, tn = lax.axis_index("dp"), lax.axis_index("tensor")
    core, z, xh = lax.rem(dp, 2), lax.rem(lax.div(dp, 2), 8), lax.div(dp, 16)
    y, xl = lax.div(tn, 2), lax.rem(tn, 2)

    def device(h, k, c, t):
        return (h * 16 + k * 2 + c, t)

    def ring(value, size):
        return lax.rem(value + size, size)

    z_up = device(xh, ring(z + 1, 8), core, tn)
    z_dn = device(xh, ring(z - 1, 8), core, tn)
    x_far = device(1 - xh, z, core, tn)
    x_near = device(xh, z, core, y * 2 + 1 - xl)
    y_up = device(xh, z, core, ring(y + 1, 4) * 2 + xl)
    y_dn = device(xh, z, core, ring(y - 1, 4) * 2 + xl)
    other = device(xh, z, 1 - core, tn)

    def unit(h, k):
        return h * 8 + ring(k, 8)

    me = unit(xh, z)
    block = xh * 4 + lax.div(z, 2)
    inside = (block == tn).astype(jnp.int32)

    barrier = pltpu.get_barrier_semaphore()

    def greet(target):
        pl.semaphore_signal(barrier, inc=1, device_id=target, device_id_type=pl.DeviceIdType.MESH)

    for target in (z_up, z_dn, x_far, x_near, y_up, y_dn, other):
        greet(target)
    for h in range(2):
        for k in range(8):
            @pl.when(jnp.logical_or(inside == 0, me != h * 8 + k))
            def _():
                greet(device(h, k, core, block))

    up_grad = (
        grad_ref[...].astype(jnp.float32) * jax.nn.silu(gate_ref[...].astype(jnp.float32))
    ).astype(jnp.bfloat16)
    rows[me] = up_grad.T

    pl.semaphore_wait(barrier, 23 - inside)

    sent = []

    def copy(src, dst, recv, target):
        made = pltpu.make_async_remote_copy(
            src_ref=src, dst_ref=dst, send_sem=ssem.at[len(sent)], recv_sem=recv,
            device_id=target, device_id_type=pl.DeviceIdType.MESH,
        )
        sent.append(None)
        return made

    waits = []

    def send(src, dst, recv, target):
        made = copy(src, dst, recv, target)
        made.start()
        waits.append(made.wait_send)

    def send_when(cond, src, dst, recv, target):
        made = copy(src, dst, recv, target)
        pl.when(cond)(made.start)
        waits.append(lambda: pl.when(cond)(made.wait_send))

    def arrive(ref, recv):
        pltpu.make_async_remote_copy(
            src_ref=ref, dst_ref=ref, send_sem=ssem.at[0], recv_sem=recv,
            device_id=other, device_id_type=pl.DeviceIdType.MESH,
        ).wait_recv()

    half_x, half_p = lax.div(tn, 4), lax.rem(tn, 4)
    for m in range(2):
        target_z = half_p * 2 + m
        for e in range(8):
            src = rows.at[me, pl.ds(m * 896 + e * PIECE, PIECE)]
            mine = jnp.logical_and(me == unit(half_x, target_z), tn == e)
            send_when(
                jnp.logical_not(mine), src, cols.at[e, me], spread_recv.at[me],
                device(half_x, target_z, core, e),
            )

            @pl.when(mine)
            def _():
                cols[e, me] = rows[me, pl.ds(m * 896 + e * PIECE, PIECE), :]

    def row(kind, u, *targets):
        ref = rows.at[u, SPAN[kind]]
        for target in targets:
            send(ref, ref, row_recv.at[kind, u], target)
        send(ref, rows_o.at[u, SPAN[kind]], rowo_recv.at[kind, u], other)

    def row_in(kind, u, *targets):
        arrive(rows.at[u, SPAN[kind]], row_recv.at[kind, u])
        row(kind, u, *targets)

    def piece(e, *targets):
        for target in targets:
            send(cols.at[e], cols.at[e], piece_recv.at[e], target)
        slot = lax.rem(e, 4)
        send_when(lax.div(e, 4) != core, cols.at[e], cols_o.at[slot], colo_recv.at[slot], other)

    def piece_in(e, *targets):
        arrive(cols.at[e], piece_recv.at[e])
        piece(e, *targets)

    row(B, me, x_far, z_up, z_dn)
    row(A, me, x_far, z_up, z_dn)

    for u in range(UNITS):
        @pl.when(jnp.logical_or(inside == 0, me != u))
        def _():
            arrive(cols.at[tn, u], spread_recv.at[u])
    piece(tn, x_near, y_up, y_dn)

    far = unit(1 - xh, z)
    row_in(B, far, z_up, z_dn)
    row_in(A, far)

    near_piece = y * 2 + 1 - xl
    dn, up, opp = ring(y - 1, 4) * 2, ring(y + 1, 4) * 2, ring(y + 2, 4) * 2
    for j in range(1, 4):
        lo, hi = unit(xh, z - j), unit(xh, z + j)
        far_lo, far_hi = unit(1 - xh, z - j), unit(1 - xh, z + j)
        row_in(B, lo, *((z_up,) if j < 3 else ()))
        row_in(B, hi, z_dn)
        row_in(A, lo, x_far, z_up)
        row_in(A, hi, x_far, *((z_dn,) if j < 3 else ()))
        if j == 1:
            piece_in(near_piece, y_up, y_dn)
        if j == 2:
            piece_in(dn + xl, y_up)
            piece_in(up + xl)
        if j == 3:
            piece_in(dn + 1 - xl)
            piece_in(up + 1 - xl, y_dn)
        row_in(B, far_lo, z_up)
        row_in(B, far_hi, *((z_dn,) if j < 3 else ()))
        if j > 1:
            row_in(A, unit(1 - xh, z - j + 1))
            row_in(A, unit(1 - xh, z + j - 1))

    piece_in(opp + xl)
    piece_in(opp + 1 - xl)

    def ready(units):
        for u in units:
            for kind in (A, B):
                arrive(rows_o.at[u, SPAN[kind]], rowo_recv.at[kind, u])

    def multiply(units, first=False, last=False):
        ready(units)
        right = jnp.concatenate(
            [
                panel.reshape(COLS, TOK)
                for u in units
                for panel in (cols[pl.ds(core * 4, 4), u], cols_o[:, u])
            ],
            axis=1,
        )

        def tile(i, _):
            span = pl.ds(pl.multiple_of(i * TILE, TILE), TILE)
            left = jnp.concatenate([r[u, span, :] for u in units for r in (rows, rows_o)], axis=1)
            total = lax.dot_general(left, right, NT, preferred_element_type=jnp.float32)
            if not first:
                total = total + out_ref[span, :]
            if last:
                total = total * (1.0 / 4096)
            out_ref[span, :] = total
            return 0

        lax.fori_loop(0, WIDTH // TILE, tile, 0)

    for slot in range(4):
        arrive(cols_o.at[slot], colo_recv.at[slot])

    def around(j):
        return [unit(h, k) for h in (xh, 1 - xh) for k in (z - j, z + j)]

    multiply([me, far], first=True)
    multiply(around(1))
    multiply(around(2))
    last, far_last = unit(xh, z + 4), unit(1 - xh, z + 4)
    row_in(A, last, x_far)
    row_in(B, last)
    row_in(B, far_last)
    row_in(A, unit(1 - xh, z - 3))
    row_in(A, unit(1 - xh, z + 3))
    multiply(around(3))
    row_in(A, far_last)
    multiply([last, far_last], last=True)

    for wait in waits:
        wait()


def shards(grad_hidden, gate):
    vmem = pl.BlockSpec(memory_space=pltpu.VMEM)
    return pl.pallas_call(
        kernel,
        out_shape=jax.ShapeDtypeStruct((WIDTH, COLS), jnp.float32),
        in_specs=[vmem] * 2,
        out_specs=vmem,
        scratch_shapes=[
            pltpu.VMEM((UNITS, WIDTH, TOK), jnp.bfloat16),
            pltpu.VMEM((UNITS, WIDTH, TOK), jnp.bfloat16),
            pltpu.VMEM((8, UNITS, PIECE, TOK), jnp.bfloat16),
            pltpu.VMEM((4, UNITS, PIECE, TOK), jnp.bfloat16),
            pltpu.SemaphoreType.DMA((2, UNITS)),
            pltpu.SemaphoreType.DMA((2, UNITS)),
            pltpu.SemaphoreType.DMA((UNITS,)),
            pltpu.SemaphoreType.DMA((8,)),
            pltpu.SemaphoreType.DMA((4,)),
            pltpu.SemaphoreType.DMA((128,)),
        ],
        compiler_params=pltpu.CompilerParams(
            collective_id=0, has_side_effects=True, vmem_limit_bytes=56 * 1024 * 1024
        ),
    )(grad_hidden, gate)


def solution(mesh):
    return jax.shard_map(
        shards,
        mesh=mesh,
        in_specs=(P("dp", "tensor"), P("dp", "tensor")),
        out_specs=P("tensor", "dp"),
        check_vma=False,
    )
```

```python
import jax
import jax.numpy as jnp
from jax import lax
from jax.experimental import pallas as pl
from jax.experimental.pallas import tpu as pltpu
from jax.sharding import PartitionSpec as P

WIDTH = 1792
TOK = 128
UNITS = 16
PIECE = 112
COLS = 448
CUT = 896
A, B = 0, 1
SPAN = (pl.ds(0, CUT), pl.ds(CUT, WIDTH - CUT))
TILE = 896
NT = (((1,), (1,)), ((), ()))


def kernel(
    grad_ref, gate_ref, out_ref, rows, rows_o, cols, cols_o, stage,
    row_recv, rowo_recv, stage_recv, spread_recv, piece_recv, colo_recv, ssem,
):
    dp, tn = lax.axis_index("dp"), lax.axis_index("tensor")
    core, z, xh = lax.rem(dp, 2), lax.rem(lax.div(dp, 2), 8), lax.div(dp, 16)
    y, xl = lax.div(tn, 2), lax.rem(tn, 2)

    def device(h, k, c, t):
        return (h * 16 + k * 2 + c, t)

    def ring(value, size):
        return lax.rem(value + size, size)

    z_up = device(xh, ring(z + 1, 8), core, tn)
    z_dn = device(xh, ring(z - 1, 8), core, tn)
    x_far = device(1 - xh, z, core, tn)
    x_near = device(xh, z, core, y * 2 + 1 - xl)
    y_up = device(xh, z, core, ring(y + 1, 4) * 2 + xl)
    y_dn = device(xh, z, core, ring(y - 1, 4) * 2 + xl)
    other = device(xh, z, 1 - core, tn)

    def unit(h, k):
        return h * 8 + ring(k, 8)

    me = unit(xh, z)
    barrier = pltpu.get_barrier_semaphore()

    def greet(target):
        pl.semaphore_signal(barrier, inc=1, device_id=target, device_id_type=pl.DeviceIdType.MESH)

    def chip(t):
        return device(lax.div(t, 8), lax.rem(t, 8), core, tn)

    greet(other)
    for step in range(1, 8):
        greet(device(xh, z, core, ring(tn + step, 8)))
    for step in range(1, UNITS):
        greet(chip(ring(me + step, UNITS)))

    up_grad = (
        grad_ref[...].astype(jnp.float32) * jax.nn.silu(gate_ref[...].astype(jnp.float32))
    ).astype(jnp.bfloat16)
    rows[me] = up_grad.T

    pl.semaphore_wait(barrier, 23)

    sent = []

    def copy(src, dst, recv, target):
        made = pltpu.make_async_remote_copy(
            src_ref=src, dst_ref=dst, send_sem=ssem.at[len(sent)], recv_sem=recv,
            device_id=target, device_id_type=pl.DeviceIdType.MESH,
        )
        sent.append(None)
        return made

    waits = []

    def send(src, dst, recv, target):
        made = copy(src, dst, recv, target)
        made.start()
        waits.append(made.wait_send)

    def send_when(cond, src, dst, recv, target):
        made = copy(src, dst, recv, target)
        pl.when(cond)(made.start)
        waits.append(lambda: pl.when(cond)(made.wait_send))

    def arrive(ref, recv):
        pltpu.make_async_remote_copy(
            src_ref=ref, dst_ref=ref, send_sem=ssem.at[0], recv_sem=recv,
            device_id=other, device_id_type=pl.DeviceIdType.MESH,
        ).wait_recv()

    def row(kind, u, *targets):
        ref = rows.at[u, SPAN[kind]]
        for target in targets:
            send(ref, ref, row_recv.at[kind, u], target)
        send(ref, rows_o.at[u, SPAN[kind]], rowo_recv.at[kind, u], other)

    def row_in(kind, u, *targets):
        arrive(rows.at[u, SPAN[kind]], row_recv.at[kind, u])
        row(kind, u, *targets)

    def half(h):
        return pl.ds(h * 8, 8)

    def piece(e, h, *targets):
        src = cols.at[e, half(h)]
        for target in targets:
            send(src, src, piece_recv.at[e, h], target)
        slot = lax.rem(e, 4)
        send_when(
            lax.div(e, 4) != core, src, cols_o.at[slot, half(h)], colo_recv.at[slot, h], other
        )

    def piece_in(e, h, *targets):
        arrive(cols.at[e, half(h)], piece_recv.at[e, h])
        piece(e, h, *targets)

    def part(m, e):
        return pl.ds(pl.multiple_of(m * 896 + e * PIECE, PIECE), PIECE)

    for step in range(1, 8):
        e = ring(tn + step, 8)
        for m in range(2):
            send(
                rows.at[me, part(m, e)], stage.at[tn * 2 + m], stage_recv.at[tn * 2 + m],
                device(xh, z, core, e),
            )
    row(B, me, x_far, z_up, z_dn)
    for m in range(2):
        stage[tn * 2 + m] = rows[me, part(m, tn), :]

    def near(j):
        return unit(xh, z - j), unit(xh, z + j)

    def across(j):
        return unit(1 - xh, z - j), unit(1 - xh, z + j)

    def rows_b(pair, last=False):
        row_in(B, pair[0], *(() if last else (z_up,)))
        row_in(B, pair[1], z_dn)

    def rows_a(pair, last=False):
        row_in(A, pair[0], x_far, z_up)
        row_in(A, pair[1], x_far, *(() if last else (z_dn,)))

    def rows_far(pair, last=False):
        row_in(B, pair[0], z_up)
        row_in(B, pair[1], *(() if last else (z_dn,)))

    def rows_end(pair):
        row_in(A, pair[0])
        row_in(A, pair[1])

    for step in range(1, 8):
        e = ring(tn + step, 8)
        for m in range(2):
            arrive(stage.at[e * 2 + m], stage_recv.at[e * 2 + m])
    for step in range(1, 8):
        t = unit(xh, z + step)
        send(stage.at[t], cols.at[tn, me], spread_recv.at[me], chip(t))
    for step in range(8):
        t = unit(1 - xh, z + step)
        send(stage.at[t], cols.at[tn, me], spread_recv.at[me], chip(t))
    row(A, me, x_far, z_up, z_dn)
    cols[tn, me] = stage[me]

    far = unit(1 - xh, z)
    near_piece = y * 2 + 1 - xl
    dn, up, opp = ring(y - 1, 4) * 2, ring(y + 1, 4) * 2, ring(y + 2, 4) * 2

    def spread(h, first):
        for step in range(first, 8):
            u = unit(h, z + step)
            arrive(cols.at[tn, u], spread_recv.at[u])
        piece(tn, h, x_near, y_up, y_dn)

    def hop(h):
        piece_in(dn + xl, h, y_up)
        piece_in(up + xl, h)
        piece_in(dn + 1 - xl, h)
        piece_in(up + 1 - xl, h, y_dn)

    def end(h):
        piece_in(opp + xl, h)
        piece_in(opp + 1 - xl, h)

    rows_b(near(1))
    row_in(B, far, z_up, z_dn)
    spread(xh, 1)
    spread(1 - xh, 0)
    rows_a(near(1))
    rows_b(near(2))
    piece_in(near_piece, xh, y_up, y_dn)
    rows_far(across(1))
    piece_in(near_piece, 1 - xh, y_up, y_dn)
    rows_a(near(2))
    row_in(A, far)
    hop(xh)
    rows_b(near(3), last=True)
    rows_end(across(1))
    hop(1 - xh)
    rows_far(across(2))
    rows_end(across(2))

    last, far_last = unit(xh, z + 4), unit(1 - xh, z + 4)
    def ready(units):
        for u in units:
            for kind in (A, B):
                arrive(rows_o.at[u, SPAN[kind]], rowo_recv.at[kind, u])

    def multiply(units, first=False, last=False):
        ready(units)
        left = jnp.concatenate(
            [
                panel.reshape(COLS, TOK)
                for u in units
                for panel in (cols[pl.ds(core * 4, 4), u], cols_o[:, u])
            ],
            axis=1,
        )

        def tile(i, _):
            span = pl.ds(pl.multiple_of(i * TILE, TILE), TILE)
            right = jnp.concatenate([r[u, span, :] for u in units for r in (rows, rows_o)], axis=1)
            total = lax.dot_general(left, right, NT, preferred_element_type=jnp.float32)
            if not first:
                total = total + out_ref[:, span]
            if last:
                total = total * (1.0 / 4096)
            out_ref[:, span] = total
            return 0

        lax.fori_loop(0, WIDTH // TILE, tile, 0)

    def around(j):
        return [unit(h, k) for h in (xh, 1 - xh) for k in (z - j, z + j)]

    end(xh)
    end(1 - xh)
    for slot in range(4):
        for h in (xh, 1 - xh):
            arrive(cols_o.at[slot, half(h)], colo_recv.at[slot, h])
    multiply([me, far], first=True)
    rows_a(near(3), last=True)
    multiply(around(1))
    rows_far(across(3), last=True)
    multiply(around(2))
    row_in(B, last)
    row_in(A, last, x_far)
    rows_end(across(3))
    row_in(B, far_last)
    multiply(around(3))
    row_in(A, far_last)
    multiply([last, far_last], last=True)

    for wait in waits:
        wait()


def shards(grad_hidden, gate):
    vmem = pl.BlockSpec(memory_space=pltpu.VMEM)
    return pl.pallas_call(
        kernel,
        out_shape=jax.ShapeDtypeStruct((COLS, WIDTH), jnp.float32),
        in_specs=[vmem] * 2,
        out_specs=vmem,
        scratch_shapes=[
            pltpu.VMEM((UNITS, WIDTH, TOK), jnp.bfloat16),
            pltpu.VMEM((UNITS, WIDTH, TOK), jnp.bfloat16),
            pltpu.VMEM((8, UNITS, PIECE, TOK), jnp.bfloat16),
            pltpu.VMEM((4, UNITS, PIECE, TOK), jnp.bfloat16),
            pltpu.VMEM((UNITS, PIECE, TOK), jnp.bfloat16),
            pltpu.SemaphoreType.DMA((2, UNITS)),
            pltpu.SemaphoreType.DMA((2, UNITS)),
            pltpu.SemaphoreType.DMA((UNITS,)),
            pltpu.SemaphoreType.DMA((UNITS,)),
            pltpu.SemaphoreType.DMA((8, 2)),
            pltpu.SemaphoreType.DMA((4, 2)),
            pltpu.SemaphoreType.DMA((160,)),
        ],
        compiler_params=pltpu.CompilerParams(
            collective_id=0, has_side_effects=True, vmem_limit_bytes=30 * 1024 * 1024
        ),
    )(grad_hidden, gate).T


def solution(mesh):
    return jax.shard_map(
        shards,
        mesh=mesh,
        in_specs=(P("dp", "tensor"), P("dp", "tensor")),
        out_specs=P("tensor", "dp"),
        check_vma=False,
    )
```

```python
import jax
import jax.numpy as jnp
from jax import lax
from jax.experimental import pallas as pl
from jax.experimental.pallas import tpu as pltpu
from jax.sharding import PartitionSpec as P

WIDTH = 1792
TOK = 128
UNITS = 16
PIECE = 112
COLS = 448
A, B, C, D = range(4)
SPAN = (pl.ds(0, 896), pl.ds(896, 896), pl.ds(896, 448), pl.ds(1344, 448))
NT = (((1,), (1,)), ((), ()))


def kernel(
    grad_hbm, gate_hbm, out_ref, grad_ref, gate_ref, rows, rows_o, cols, cols_o, stage,
    row_recv, split_recv, rowo_recv, stage_recv, spread_recv, piece_recv, colo_recv, sent, load_sem,
):
    dp, tn = lax.axis_index("dp"), lax.axis_index("tensor")
    core, z, xh = lax.rem(dp, 2), lax.rem(lax.div(dp, 2), 8), lax.div(dp, 16)
    y, xl = lax.div(tn, 2), lax.rem(tn, 2)

    def device(h, k, c, t):
        return (h * 16 + k * 2 + c, t)

    def ring(value, size):
        return lax.rem(value + size, size)

    z_up = device(xh, ring(z + 1, 8), core, tn)
    z_dn = device(xh, ring(z - 1, 8), core, tn)
    x_far = device(1 - xh, z, core, tn)
    x_near = device(xh, z, core, y * 2 + 1 - xl)
    y_up = device(xh, z, core, ring(y + 1, 4) * 2 + xl)
    y_dn = device(xh, z, core, ring(y - 1, 4) * 2 + xl)
    other = device(xh, z, 1 - core, tn)

    def unit(h, k):
        return h * 8 + ring(k, 8)

    me = unit(xh, z)
    loads = [
        pltpu.make_async_copy(src, dst, load_sem.at[i])
        for i, (src, dst) in enumerate(((grad_hbm, grad_ref), (gate_hbm, gate_ref)))
    ]
    for load in loads:
        load.start()

    barrier = pltpu.get_barrier_semaphore()

    def greet(target):
        pl.semaphore_signal(barrier, inc=1, device_id=target, device_id_type=pl.DeviceIdType.MESH)

    def chip(t):
        return device(lax.div(t, 8), lax.rem(t, 8), core, tn)

    greet(other)
    for step in range(1, 8):
        greet(device(xh, z, core, ring(tn + step, 8)))
    for step in range(1, UNITS):
        greet(chip(ring(me + step, UNITS)))

    for load in loads:
        load.wait()
    up_grad = (
        grad_ref[...].astype(jnp.float32) * jax.nn.silu(gate_ref[...].astype(jnp.float32))
    ).astype(jnp.bfloat16)
    rows[me] = up_grad.T

    pl.semaphore_wait(barrier, 23)

    ROW, ROW_O, SCATTER, SPREAD, PLANE, PLANE_O = (sent.at[i] for i in range(6))

    def copy(src, dst, send, recv, target):
        return pltpu.make_async_remote_copy(
            src_ref=src, dst_ref=dst, send_sem=send, recv_sem=recv,
            device_id=target, device_id_type=pl.DeviceIdType.MESH,
        )

    def arrive(ref, recv):
        copy(ref, ref, sent.at[0], recv, other).wait_recv()

    def leave(ref, send):
        copy(ref, ref, send, load_sem.at[0], other).wait_send()

    def pass_on(kind, u, *targets, recv=None):
        ref = rows.at[u, SPAN[kind]]
        for target in targets:
            copy(ref, ref, ROW, row_recv.at[kind, u] if recv is None else recv, target).start()

    def share(kind, u, group):
        copy(
            rows.at[u, SPAN[kind]], rows_o.at[u, SPAN[kind]], ROW_O,
            rowo_recv.at[min(kind, B), group], other,
        ).start()

    def row_in(kind, u, group, *targets):
        arrive(rows.at[u, SPAN[kind]], row_recv.at[kind, u])
        pass_on(kind, u, *targets)
        share(kind, u, group)

    def half(h):
        return pl.ds(h * 8, 8)

    def piece(e, h, *targets):
        src = cols.at[e, half(h)]
        for target in targets:
            copy(src, src, PLANE, piece_recv.at[e, h], target).start()

        @pl.when(lax.div(e, 4) != core)
        def _():
            copy(src, cols_o.at[lax.rem(e, 4), half(h)], PLANE_O, colo_recv, other).start()

    def piece_in(e, h, *targets):
        arrive(cols.at[e, half(h)], piece_recv.at[e, h])
        piece(e, h, *targets)

    def part(m, e):
        return pl.ds(pl.multiple_of(m * 896 + e * PIECE, PIECE), PIECE)

    for step in range(1, 8):
        e = ring(tn + step, 8)
        for m in range(2):
            copy(
                rows.at[me, part(m, e)], stage.at[tn * 2 + m], SCATTER, stage_recv,
                device(xh, z, core, e),
            ).start()
    pass_on(A, me, z_up, z_dn)
    pass_on(B, me, x_far)
    pass_on(C, me, z_up, recv=split_recv.at[0, 0])
    pass_on(C, me, z_dn, recv=split_recv.at[0, 1])
    pass_on(A, me, x_far)
    share(A, me, 0)
    share(B, me, 0)
    for m in range(2):
        stage[tn * 2 + m] = rows[me, part(m, tn), :]

    arrive(stage.at[pl.ds(0, 14)], stage_recv)
    for h, first in ((xh, 1), (1 - xh, 0)):
        for step in range(first, 8):
            t = unit(h, z + step)
            copy(stage.at[t], cols.at[tn, me], SPREAD, spread_recv.at[first], chip(t)).start()
    pass_on(D, me, z_up, recv=split_recv.at[1, 0])
    pass_on(D, me, z_dn, recv=split_recv.at[1, 1])
    cols[tn, me] = stage[me]

    far, last, far_last = unit(1 - xh, z), unit(xh, z + 4), unit(1 - xh, z + 4)
    near_piece = y * 2 + 1 - xl
    dn, up, opp = ring(y - 1, 4) * 2, ring(y + 1, 4) * 2, ring(y + 2, 4) * 2

    def lo(j):
        return unit(xh, z - j)

    def hi(j):
        return unit(xh, z + j)

    def far_lo(j):
        return unit(1 - xh, z - j)

    def far_hi(j):
        return unit(1 - xh, z + j)

    def spread(h, first):
        arrive(stage.at[pl.ds(0, 8 - first)], spread_recv.at[first])
        piece(tn, h, x_near, y_up, y_dn)

    def hop(h):
        piece_in(dn + xl, h, y_up)
        piece_in(up + xl, h)
        piece_in(dn + 1 - xl, h)
        piece_in(up + 1 - xl, h, y_dn)

    def end(h):
        piece_in(opp + xl, h)
        piece_in(opp + 1 - xl, h)

    def split_in(u, side, target):
        arrive(rows.at[u, SPAN[C]], split_recv.at[0, side])
        arrive(rows.at[u, SPAN[D]], split_recv.at[1, side])
        pass_on(B, u, target)
        share(B, u, 0)

    groups = [[me, far]] + [[lo(j), hi(j), far_lo(j), far_hi(j)] for j in range(1, 4)]
    groups = [groups[0] + groups[1], groups[2], groups[3], [last, far_last]]

    def multiply(kind, g):
        units = groups[g]
        arrive(rows_o.at[pl.ds(0, len(units) // 2)], rowo_recv.at[kind, g])
        left = jnp.concatenate(
            [
                panel.reshape(COLS, TOK)
                for u in units
                for panel in (cols[pl.ds(core * 4, 4), u], cols_o[:, u])
            ],
            axis=1,
        )
        right = jnp.concatenate([r[u, SPAN[kind], :] for u in units for r in (rows, rows_o)], axis=1)
        total = lax.dot_general(left, right, NT, preferred_element_type=jnp.float32)
        if g > 0:
            total = total + out_ref[:, SPAN[kind]]
        if g == 3:
            total = total * (1.0 / 4096)
        out_ref[:, SPAN[kind]] = total

    row_in(A, lo(1), 0, z_up)
    row_in(A, hi(1), 0, z_dn)
    row_in(B, far, 0, z_up, z_dn)
    spread(xh, 1)
    spread(1 - xh, 0)
    pass_on(A, lo(1), x_far)
    pass_on(A, hi(1), x_far)
    row_in(A, far, 0)
    piece_in(near_piece, xh, y_up, y_dn)
    row_in(A, lo(2), 1, z_up, x_far)
    row_in(A, hi(2), 1, z_dn, x_far)
    piece_in(near_piece, 1 - xh, y_up, y_dn)
    split_in(hi(1), 1, z_dn)
    row_in(B, far_lo(1), 0, z_up)
    row_in(B, far_hi(1), 0, z_dn)
    hop(xh)
    row_in(A, lo(3), 2, z_up, x_far)
    row_in(A, hi(3), 2, x_far)
    split_in(lo(1), 0, z_up)
    hop(1 - xh)
    row_in(A, far_lo(1), 0)
    row_in(A, far_hi(1), 0)
    row_in(B, hi(2), 1, z_dn)
    row_in(B, far_lo(2), 1, z_up)
    end(xh)
    row_in(B, far_hi(2), 1, z_dn)
    row_in(A, last, 3, x_far)
    end(1 - xh)
    arrive(cols_o, colo_recv)
    multiply(A, 0)
    row_in(B, lo(2), 1, z_up)
    row_in(A, far_lo(2), 1)
    row_in(A, far_hi(2), 1)
    multiply(B, 0)
    row_in(B, hi(3), 2, z_dn)
    multiply(A, 1)
    row_in(B, far_lo(3), 2)
    pass_on(C, far_lo(3), z_up, recv=split_recv.at[0, 2])
    row_in(B, far_hi(3), 2)
    pass_on(D, far_hi(3), z_dn, recv=split_recv.at[1, 2])
    multiply(B, 1)
    row_in(A, far_lo(3), 2)
    row_in(A, far_hi(3), 2)
    multiply(A, 2)
    row_in(B, lo(3), 2)
    row_in(B, last, 3)
    row_in(A, far_last, 3)
    for kind in (C, D):
        arrive(rows.at[far_last, SPAN[kind]], split_recv.at[kind - C, 2])
        share(kind, far_last, 3)
    multiply(B, 2)
    multiply(A, 3)
    multiply(B, 3)

    leave(rows.at[pl.ds(0, 15)], ROW)
    leave(rows, ROW_O)
    leave(stage.at[pl.ds(0, 14)], SCATTER)
    leave(stage.at[pl.ds(0, 15)], SPREAD)
    leave(cols.at[pl.ds(0, 7)], PLANE)
    leave(cols_o, PLANE_O)


def shards(grad_hidden, gate):
    dma = pltpu.SemaphoreType.DMA
    return pl.pallas_call(
        kernel,
        out_shape=jax.ShapeDtypeStruct((COLS, WIDTH), jnp.float32),
        in_specs=[pl.BlockSpec(memory_space=pltpu.HBM)] * 2,
        out_specs=pl.BlockSpec(memory_space=pltpu.VMEM),
        scratch_shapes=[
            pltpu.VMEM((TOK, WIDTH), jnp.bfloat16),
            pltpu.VMEM((TOK, WIDTH), jnp.bfloat16),
            pltpu.VMEM((UNITS, WIDTH, TOK), jnp.bfloat16),
            pltpu.VMEM((UNITS, WIDTH, TOK), jnp.bfloat16),
            pltpu.VMEM((8, UNITS, PIECE, TOK), jnp.bfloat16),
            pltpu.VMEM((4, UNITS, PIECE, TOK), jnp.bfloat16),
            pltpu.VMEM((UNITS, PIECE, TOK), jnp.bfloat16),
            dma((2, UNITS)),
            dma((2, 3)),
            dma((2, 4)),
            dma,
            dma((2,)),
            dma((8, 2)),
            dma,
            dma((6,)),
            dma((2,)),
        ],
        compiler_params=pltpu.CompilerParams(
            collective_id=0, has_side_effects=True, vmem_limit_bytes=40_000_000
        ),
    )(*(pltpu.with_memory_space_constraint(a, pltpu.HBM) for a in (grad_hidden, gate))).T


def solution(mesh):
    return jax.shard_map(
        shards,
        mesh=mesh,
        in_specs=(P("dp", "tensor"), P("dp", "tensor")),
        out_specs=P("tensor", "dp"),
        check_vma=False,
    )
```

```python
import jax
import jax.numpy as jnp
from jax import lax
from jax.experimental import pallas as pl
from jax.experimental.pallas import tpu as pltpu
from jax.sharding import PartitionSpec as P

WIDTH = 1792
TOK = 128
UNITS = 16
PIECE = 112
COLS = 448
A, B, C, D = range(4)
CUT, HALF = 864, 464
SPAN = (pl.ds(0, CUT), pl.ds(CUT, 2 * HALF), pl.ds(CUT, HALF), pl.ds(CUT + HALF, HALF))
PART = (pl.ds(0, 768), pl.ds(768, WIDTH - 768))
NT = (((1,), (1,)), ((), ()))


def kernel(
    grad_hbm, gate_hbm, out_ref, grad_ref, gate_ref, rows, rows_o, cols, cols_o, stage,
    row_recv, split_recv, rowo_recv, stage_recv, spread_recv, piece_recv, colo_recv, sent, load_sem,
):
    dp, tn = lax.axis_index("dp"), lax.axis_index("tensor")
    core, z, xh = lax.rem(dp, 2), lax.rem(lax.div(dp, 2), 8), lax.div(dp, 16)
    y, xl = lax.div(tn, 2), lax.rem(tn, 2)

    def device(h, k, c, t):
        return (h * 16 + k * 2 + c, t)

    def ring(value, size):
        return lax.rem(value + size, size)

    z_up = device(xh, ring(z + 1, 8), core, tn)
    z_dn = device(xh, ring(z - 1, 8), core, tn)
    x_far = device(1 - xh, z, core, tn)
    x_near = device(xh, z, core, y * 2 + 1 - xl)
    y_up = device(xh, z, core, ring(y + 1, 4) * 2 + xl)
    y_dn = device(xh, z, core, ring(y - 1, 4) * 2 + xl)
    other = device(xh, z, 1 - core, tn)

    def unit(h, k):
        return h * 8 + ring(k, 8)

    me = unit(xh, z)
    loads = [
        pltpu.make_async_copy(src, dst, load_sem.at[i])
        for i, (src, dst) in enumerate(((grad_hbm, grad_ref), (gate_hbm, gate_ref)))
    ]
    for load in loads:
        load.start()

    barrier = pltpu.get_barrier_semaphore()

    def greet(target):
        pl.semaphore_signal(barrier, inc=1, device_id=target, device_id_type=pl.DeviceIdType.MESH)

    def chip(t):
        return device(lax.div(t, 8), lax.rem(t, 8), core, tn)

    greet(other)
    for step in range(1, 8):
        greet(device(xh, z, core, ring(tn + step, 8)))
    for step in range(1, UNITS):
        greet(chip(ring(me + step, UNITS)))

    for load in loads:
        load.wait()
    up_grad = (
        grad_ref[...].astype(jnp.float32) * jax.nn.silu(gate_ref[...].astype(jnp.float32))
    ).astype(jnp.bfloat16)
    rows[me] = up_grad.T

    pl.semaphore_wait(barrier, 23)

    ROW, ROW_O, SCATTER, SPREAD, PLANE, PLANE_O = (sent.at[i] for i in range(6))

    def copy(src, dst, send, recv, target):
        return pltpu.make_async_remote_copy(
            src_ref=src, dst_ref=dst, send_sem=send, recv_sem=recv,
            device_id=target, device_id_type=pl.DeviceIdType.MESH,
        )

    def arrive(ref, recv):
        copy(ref, ref, sent.at[0], recv, other).wait_recv()

    def leave(ref, send):
        copy(ref, ref, send, load_sem.at[0], other).wait_send()

    def pass_on(kind, u, *targets, recv=None):
        ref = rows.at[u, SPAN[kind]]
        for target in targets:
            copy(ref, ref, ROW, row_recv.at[kind, u] if recv is None else recv, target).start()

    def share(kind, u, group):
        copy(
            rows.at[u, SPAN[kind]], rows_o.at[u, SPAN[kind]], ROW_O,
            rowo_recv.at[min(kind, B), group], other,
        ).start()

    def row_in(kind, u, group, *targets):
        arrive(rows.at[u, SPAN[kind]], row_recv.at[kind, u])
        pass_on(kind, u, *targets)
        share(kind, u, group)

    def half(h):
        return pl.ds(h * 8, 8)

    def piece(e, h, *targets):
        src = cols.at[e, half(h)]
        for target in targets:
            copy(src, src, PLANE, piece_recv.at[e, h], target).start()

        @pl.when(lax.div(e, 4) != core)
        def _():
            copy(src, cols_o.at[lax.rem(e, 4), half(h)], PLANE_O, colo_recv, other).start()

    def piece_in(e, h, *targets):
        arrive(cols.at[e, half(h)], piece_recv.at[e, h])
        piece(e, h, *targets)

    def part(m, e):
        return pl.ds(pl.multiple_of(m * 896 + e * PIECE, PIECE), PIECE)

    for step in range(1, 8):
        e = ring(tn + step, 8)
        for m in range(2):
            copy(
                rows.at[me, part(m, e)], stage.at[tn * 2 + m], SCATTER, stage_recv,
                device(xh, z, core, e),
            ).start()
    pass_on(A, me, z_up, z_dn)
    pass_on(B, me, x_far)
    pass_on(C, me, z_up, recv=split_recv.at[0, 0])
    pass_on(C, me, z_dn, recv=split_recv.at[0, 1])
    pass_on(A, me, x_far)
    share(A, me, 0)
    share(B, me, 0)
    for m in range(2):
        stage[tn * 2 + m] = rows[me, part(m, tn), :]

    arrive(stage.at[pl.ds(0, 14)], stage_recv)
    for h, first in ((xh, 1), (1 - xh, 0)):
        for step in range(first, 8):
            t = unit(h, z + step)
            copy(stage.at[t], cols.at[tn, me], SPREAD, spread_recv.at[first], chip(t)).start()
    pass_on(D, me, z_up, recv=split_recv.at[1, 0])
    pass_on(D, me, z_dn, recv=split_recv.at[1, 1])
    cols[tn, me] = stage[me]

    far, last, far_last = unit(1 - xh, z), unit(xh, z + 4), unit(1 - xh, z + 4)
    near_piece = y * 2 + 1 - xl
    dn, up, opp = ring(y - 1, 4) * 2, ring(y + 1, 4) * 2, ring(y + 2, 4) * 2

    def lo(j):
        return unit(xh, z - j)

    def hi(j):
        return unit(xh, z + j)

    def far_lo(j):
        return unit(1 - xh, z - j)

    def far_hi(j):
        return unit(1 - xh, z + j)

    def spread(h, first):
        arrive(stage.at[pl.ds(0, 8 - first)], spread_recv.at[first])
        piece(tn, h, x_near, y_up, y_dn)

    def hop(h):
        piece_in(dn + xl, h, y_up)
        piece_in(up + xl, h)
        piece_in(dn + 1 - xl, h)
        piece_in(up + 1 - xl, h, y_dn)

    def end(h):
        piece_in(opp + xl, h)
        piece_in(opp + 1 - xl, h)

    def split_in(u, side, target):
        arrive(rows.at[u, SPAN[C]], split_recv.at[0, side])
        arrive(rows.at[u, SPAN[D]], split_recv.at[1, side])
        pass_on(B, u, target)
        share(B, u, 0)

    groups = [[me, far]] + [[lo(j), hi(j), far_lo(j), far_hi(j)] for j in range(1, 4)]
    groups = [groups[0] + groups[1], groups[2], groups[3], [last, far_last]]

    def multiply(kind, g):
        units = groups[g]
        arrive(rows_o.at[pl.ds(0, len(units)), SPAN[kind]], rowo_recv.at[kind, g])
        left = jnp.concatenate(
            [
                panel.reshape(COLS, TOK)
                for u in units
                for panel in (cols[pl.ds(core * 4, 4), u], cols_o[:, u])
            ],
            axis=1,
        )
        right = jnp.concatenate([r[u, PART[kind], :] for u in units for r in (rows, rows_o)], axis=1)
        total = lax.dot_general(left, right, NT, preferred_element_type=jnp.float32)
        if g > 0:
            total = total + out_ref[:, PART[kind]]
        if g == 3:
            total = total * (1.0 / 4096)
        out_ref[:, PART[kind]] = total

    row_in(A, lo(1), 0, z_up)
    row_in(A, hi(1), 0, z_dn)
    row_in(B, far, 0, z_up, z_dn)
    spread(xh, 1)
    spread(1 - xh, 0)
    pass_on(A, lo(1), x_far)
    pass_on(A, hi(1), x_far)
    row_in(A, lo(2), 1, z_up, x_far)
    row_in(A, hi(2), 1, z_dn, x_far)
    piece_in(near_piece, xh, y_up, y_dn)
    row_in(A, far, 0)
    split_in(hi(1), 1, z_dn)
    row_in(B, far_lo(1), 0, z_up)
    row_in(B, far_hi(1), 0, z_dn)
    piece_in(near_piece, 1 - xh, y_up, y_dn)
    row_in(A, lo(3), 2, z_up, x_far)
    row_in(A, hi(3), 2, x_far)
    split_in(lo(1), 0, z_up)
    hop(xh)
    row_in(B, hi(2), 1, z_dn)
    row_in(A, far_lo(1), 0)
    row_in(A, far_hi(1), 0)
    row_in(B, far_lo(2), 1, z_up)
    hop(1 - xh)
    row_in(B, far_hi(2), 1, z_dn)
    row_in(A, last, 3, x_far)
    end(xh)
    row_in(B, lo(2), 1, z_up)
    end(1 - xh)
    row_in(B, hi(3), 2, z_dn)
    arrive(cols_o, colo_recv)
    multiply(A, 0)
    row_in(A, far_lo(2), 1)
    row_in(A, far_hi(2), 1)
    multiply(B, 0)
    row_in(B, far_lo(3), 2)
    pass_on(C, far_lo(3), z_up, recv=split_recv.at[0, 2])
    row_in(B, far_hi(3), 2)
    pass_on(D, far_hi(3), z_dn, recv=split_recv.at[1, 2])
    multiply(A, 1)
    multiply(B, 1)
    row_in(A, far_lo(3), 2)
    row_in(A, far_hi(3), 2)
    row_in(B, lo(3), 2)
    row_in(B, last, 3)
    multiply(A, 2)
    row_in(A, far_last, 3)
    for kind in (C, D):
        arrive(rows.at[far_last, SPAN[kind]], split_recv.at[kind - C, 2])
        share(kind, far_last, 3)
    multiply(B, 2)
    multiply(A, 3)
    multiply(B, 3)

    leave(rows.at[pl.ds(0, 15)], ROW)
    leave(rows, ROW_O)
    leave(stage.at[pl.ds(0, 14)], SCATTER)
    leave(stage.at[pl.ds(0, 15)], SPREAD)
    leave(cols.at[pl.ds(0, 7)], PLANE)
    leave(cols_o, PLANE_O)


def shards(grad_hidden, gate):
    dma = pltpu.SemaphoreType.DMA
    return pl.pallas_call(
        kernel,
        out_shape=jax.ShapeDtypeStruct((COLS, WIDTH), jnp.float32),
        in_specs=[pl.BlockSpec(memory_space=pltpu.HBM)] * 2,
        out_specs=pl.BlockSpec(memory_space=pltpu.VMEM),
        scratch_shapes=[
            pltpu.VMEM((TOK, WIDTH), jnp.bfloat16),
            pltpu.VMEM((TOK, WIDTH), jnp.bfloat16),
            pltpu.VMEM((UNITS, WIDTH, TOK), jnp.bfloat16),
            pltpu.VMEM((UNITS, WIDTH, TOK), jnp.bfloat16),
            pltpu.VMEM((8, UNITS, PIECE, TOK), jnp.bfloat16),
            pltpu.VMEM((4, UNITS, PIECE, TOK), jnp.bfloat16),
            pltpu.VMEM((UNITS, PIECE, TOK), jnp.bfloat16),
            dma((2, UNITS)),
            dma((2, 3)),
            dma((2, 4)),
            dma,
            dma((2,)),
            dma((8, 2)),
            dma,
            dma((6,)),
            dma((2,)),
        ],
        compiler_params=pltpu.CompilerParams(
            collective_id=0, has_side_effects=True, vmem_limit_bytes=40_000_000
        ),
    )(*(pltpu.with_memory_space_constraint(a, pltpu.HBM) for a in (grad_hidden, gate))).T


def solution(mesh):
    return jax.shard_map(
        shards,
        mesh=mesh,
        in_specs=(P("dp", "tensor"), P("dp", "tensor")),
        out_specs=P("tensor", "dp"),
        check_vma=False,
    )
```

```python
import jax
import jax.numpy as jnp
from jax import lax
from jax.experimental import pallas as pl
from jax.experimental.pallas import tpu as pltpu
from jax.sharding import PartitionSpec as P

WIDTH = 1792
TOK = 128
UNITS = 16
PIECE = 112
COLS = 448
A, B, C, D = range(4)
CUT, HALF = 864, 464
SPAN = (pl.ds(0, CUT), pl.ds(CUT, 2 * HALF), pl.ds(CUT, HALF), pl.ds(CUT + HALF, HALF))
PART = (pl.ds(0, 768), pl.ds(768, WIDTH - 768))
NT = (((1,), (1,)), ((), ()))


def kernel(
    grad_hbm, gate_hbm, out_ref, grad_ref, gate_ref, rows, rows_o, cols, cols_o, stage,
    row_recv, split_recv, rowo_recv, stage_recv, spread_recv, piece_recv, colo_recv, sent, load_sem,
):
    dp, tn = lax.axis_index("dp"), lax.axis_index("tensor")
    core, z, xh = lax.rem(dp, 2), lax.rem(lax.div(dp, 2), 8), lax.div(dp, 16)
    y, xl = lax.div(tn, 2), lax.rem(tn, 2)

    def device(h, k, c, t):
        return (h * 16 + k * 2 + c, t)

    def ring(value, size):
        return lax.rem(value + size, size)

    z_up = device(xh, ring(z + 1, 8), core, tn)
    z_dn = device(xh, ring(z - 1, 8), core, tn)
    x_far = device(1 - xh, z, core, tn)
    x_near = device(xh, z, core, y * 2 + 1 - xl)
    y_up = device(xh, z, core, ring(y + 1, 4) * 2 + xl)
    y_dn = device(xh, z, core, ring(y - 1, 4) * 2 + xl)
    other = device(xh, z, 1 - core, tn)

    def unit(h, k):
        return h * 8 + ring(k, 8)

    me = unit(xh, z)
    loads = [
        pltpu.make_async_copy(src, dst, load_sem.at[i])
        for i, (src, dst) in enumerate(((grad_hbm, grad_ref), (gate_hbm, gate_ref)))
    ]
    for load in loads:
        load.start()

    barrier = pltpu.get_barrier_semaphore()

    def greet(target):
        pl.semaphore_signal(barrier, inc=1, device_id=target, device_id_type=pl.DeviceIdType.MESH)

    def chip(t):
        return device(lax.div(t, 8), lax.rem(t, 8), core, tn)

    greet(other)
    for step in range(1, 8):
        greet(device(xh, z, core, ring(tn + step, 8)))
    for step in range(1, UNITS):
        greet(chip(ring(me + step, UNITS)))

    for load in loads:
        load.wait()
    up_grad = (
        grad_ref[...].astype(jnp.float32) * jax.nn.silu(gate_ref[...].astype(jnp.float32))
    ).astype(jnp.bfloat16)
    rows[me] = up_grad.T

    pl.semaphore_wait(barrier, 23)

    ROW, ROW_O, SCATTER, SPREAD, PLANE, PLANE_O = (sent.at[i] for i in range(6))

    def copy(src, dst, send, recv, target):
        return pltpu.make_async_remote_copy(
            src_ref=src, dst_ref=dst, send_sem=send, recv_sem=recv,
            device_id=target, device_id_type=pl.DeviceIdType.MESH,
        )

    def arrive(ref, recv):
        copy(ref, ref, sent.at[0], recv, other).wait_recv()

    def leave(ref, send):
        copy(ref, ref, send, load_sem.at[0], other).wait_send()

    def pass_on(kind, u, *targets, recv=None):
        ref = rows.at[u, SPAN[kind]]
        for target in targets:
            copy(ref, ref, ROW, row_recv.at[kind, u] if recv is None else recv, target).start()

    def share(kind, u, group):
        copy(
            rows.at[u, SPAN[kind]], rows_o.at[u, SPAN[kind]], ROW_O,
            rowo_recv.at[min(kind, B), group], other,
        ).start()

    def row_in(kind, u, group, *targets):
        arrive(rows.at[u, SPAN[kind]], row_recv.at[kind, u])
        pass_on(kind, u, *targets)
        share(kind, u, group)

    def half(h):
        return pl.ds(h * 8, 8)

    def piece(e, h, *targets):
        src = cols.at[e, half(h)]
        for target in targets:
            copy(src, src, PLANE, piece_recv.at[e, h], target).start()

        @pl.when(lax.div(e, 4) != core)
        def _():
            copy(src, cols_o.at[lax.rem(e, 4), half(h)], PLANE_O, colo_recv, other).start()

    def piece_in(e, h, *targets):
        arrive(cols.at[e, half(h)], piece_recv.at[e, h])
        piece(e, h, *targets)

    def part(m, e):
        return pl.ds(pl.multiple_of(m * 896 + e * PIECE, PIECE), PIECE)

    for step in range(1, 8):
        e = ring(tn + step, 8)
        for m in range(2):
            copy(
                rows.at[me, part(m, e)], stage.at[tn * 2 + m], SCATTER, stage_recv,
                device(xh, z, core, e),
            ).start()
    pass_on(A, me, z_up, z_dn)
    pass_on(B, me, x_far)
    pass_on(B, me, z_up, z_dn)
    pass_on(A, me, x_far)
    share(A, me, 0)
    share(B, me, 0)
    for m in range(2):
        stage[tn * 2 + m] = rows[me, part(m, tn), :]

    arrive(stage.at[pl.ds(0, 14)], stage_recv)
    for h, first in ((xh, 1), (1 - xh, 0)):
        for step in range(first, 8):
            t = unit(h, z + step)
            copy(stage.at[t], cols.at[tn, me], SPREAD, spread_recv.at[first], chip(t)).start()
    cols[tn, me] = stage[me]

    far, last, far_last = unit(1 - xh, z), unit(xh, z + 4), unit(1 - xh, z + 4)
    near_piece = y * 2 + 1 - xl
    dn, up, opp = ring(y - 1, 4) * 2, ring(y + 1, 4) * 2, ring(y + 2, 4) * 2

    def lo(j):
        return unit(xh, z - j)

    def hi(j):
        return unit(xh, z + j)

    def far_lo(j):
        return unit(1 - xh, z - j)

    def far_hi(j):
        return unit(1 - xh, z + j)

    def spread(h, first):
        arrive(stage.at[pl.ds(0, 8 - first)], spread_recv.at[first])
        piece(tn, h, x_near, y_up, y_dn)

    def hop(h):
        piece_in(dn + xl, h, y_up)
        piece_in(up + xl, h)
        piece_in(dn + 1 - xl, h)
        piece_in(up + 1 - xl, h, y_dn)

    def end(h):
        piece_in(opp + xl, h)
        piece_in(opp + 1 - xl, h)

    groups = [[me, far]] + [[lo(j), hi(j), far_lo(j), far_hi(j)] for j in range(1, 4)]
    groups = [groups[0] + groups[1], groups[2], groups[3], [last, far_last]]

    def multiply(kind, g):
        units = groups[g]
        arrive(rows_o.at[pl.ds(0, len(units)), SPAN[kind]], rowo_recv.at[kind, g])
        left = jnp.concatenate(
            [
                panel.reshape(COLS, TOK)
                for u in units
                for panel in (cols[pl.ds(core * 4, 4), u], cols_o[:, u])
            ],
            axis=1,
        )
        right = jnp.concatenate([r[u, PART[kind], :] for u in units for r in (rows, rows_o)], axis=1)
        total = lax.dot_general(left, right, NT, preferred_element_type=jnp.float32)
        if g > 0:
            total = total + out_ref[:, PART[kind]]
        if g == 3:
            total = total * (1.0 / 4096)
        out_ref[:, PART[kind]] = total

    row_in(A, lo(1), 0, z_up)
    row_in(A, hi(1), 0, z_dn)
    row_in(B, far, 0, z_up, z_dn)
    spread(xh, 1)
    spread(1 - xh, 0)
    pass_on(A, lo(1), x_far)
    pass_on(A, hi(1), x_far)
    row_in(A, lo(2), 1, z_up, x_far)
    row_in(A, hi(2), 1, z_dn, x_far)
    piece_in(near_piece, xh, y_up, y_dn)
    row_in(A, far, 0)
    row_in(B, hi(1), 0, z_dn)
    row_in(B, far_lo(1), 0, z_up)
    row_in(B, far_hi(1), 0, z_dn)
    piece_in(near_piece, 1 - xh, y_up, y_dn)
    row_in(A, lo(3), 2, z_up, x_far)
    row_in(A, hi(3), 2, x_far)
    row_in(B, lo(1), 0, z_up)
    hop(xh)
    row_in(B, hi(2), 1, z_dn)
    row_in(A, far_lo(1), 0)
    row_in(A, far_hi(1), 0)
    row_in(B, far_lo(2), 1, z_up)
    hop(1 - xh)
    row_in(B, far_hi(2), 1, z_dn)
    row_in(A, last, 3, x_far)
    end(xh)
    row_in(B, lo(2), 1, z_up)
    end(1 - xh)
    row_in(B, hi(3), 2, z_dn)
    arrive(cols_o, colo_recv)
    multiply(A, 0)
    row_in(A, far_lo(2), 1)
    row_in(A, far_hi(2), 1)
    multiply(B, 0)
    row_in(B, far_lo(3), 2)
    pass_on(C, far_lo(3), z_up, recv=split_recv.at[0])
    row_in(B, far_hi(3), 2)
    pass_on(D, far_hi(3), z_dn, recv=split_recv.at[1])
    multiply(A, 1)
    multiply(B, 1)
    row_in(A, far_lo(3), 2)
    row_in(A, far_hi(3), 2)
    row_in(B, lo(3), 2)
    row_in(B, last, 3)
    multiply(A, 2)
    row_in(A, far_last, 3)
    for kind in (C, D):
        arrive(rows.at[far_last, SPAN[kind]], split_recv.at[kind - C])
        share(kind, far_last, 3)
    multiply(B, 2)
    multiply(A, 3)
    multiply(B, 3)

    leave(rows.at[pl.ds(0, 15)], ROW)
    leave(rows, ROW_O)
    leave(stage.at[pl.ds(0, 14)], SCATTER)
    leave(stage.at[pl.ds(0, 15)], SPREAD)
    leave(cols.at[pl.ds(0, 7)], PLANE)
    leave(cols_o, PLANE_O)


def shards(grad_hidden, gate):
    dma = pltpu.SemaphoreType.DMA
    return pl.pallas_call(
        kernel,
        out_shape=jax.ShapeDtypeStruct((COLS, WIDTH), jnp.float32),
        in_specs=[pl.BlockSpec(memory_space=pltpu.HBM)] * 2,
        out_specs=pl.BlockSpec(memory_space=pltpu.VMEM),
        scratch_shapes=[
            pltpu.VMEM((TOK, WIDTH), jnp.bfloat16),
            pltpu.VMEM((TOK, WIDTH), jnp.bfloat16),
            pltpu.VMEM((UNITS, WIDTH, TOK), jnp.bfloat16),
            pltpu.VMEM((UNITS, WIDTH, TOK), jnp.bfloat16),
            pltpu.VMEM((8, UNITS, PIECE, TOK), jnp.bfloat16),
            pltpu.VMEM((4, UNITS, PIECE, TOK), jnp.bfloat16),
            pltpu.VMEM((UNITS, PIECE, TOK), jnp.bfloat16),
            dma((2, UNITS)),
            dma((2,)),
            dma((2, 4)),
            dma,
            dma((2,)),
            dma((8, 2)),
            dma,
            dma((6,)),
            dma((2,)),
        ],
        compiler_params=pltpu.CompilerParams(
            collective_id=0, has_side_effects=True, vmem_limit_bytes=40_000_000
        ),
    )(*(pltpu.with_memory_space_constraint(a, pltpu.HBM) for a in (grad_hidden, gate))).T


def solution(mesh):
    return jax.shard_map(
        shards,
        mesh=mesh,
        in_specs=(P("dp", "tensor"), P("dp", "tensor")),
        out_specs=P("tensor", "dp"),
        check_vma=False,
    )
```

```python
import jax
import jax.numpy as jnp
from jax import lax
from jax.experimental import pallas as pl
from jax.experimental.pallas import tpu as pltpu
from jax.sharding import PartitionSpec as P

WIDTH = 1792
TOK = 128
UNITS = 16
PIECE = 112
COLS = 448
A, B, C, D = range(4)
CUT, HALF = 864, 464
SPAN = (pl.ds(0, CUT), pl.ds(CUT, 2 * HALF), pl.ds(CUT, HALF), pl.ds(CUT + HALF, HALF))
PART = (pl.ds(0, 768), pl.ds(768, WIDTH - 768))
NT = (((1,), (1,)), ((), ()))


def kernel(
    grad_hbm, gate_hbm, out_ref, grad_ref, gate_ref, rows, rows_o, cols, cols_o, stage,
    row_recv, split_recv, rowo_recv, stage_recv, spread_recv, piece_recv, colo_recv, sent, load_sem,
):
    dp, tn = lax.axis_index("dp"), lax.axis_index("tensor")
    core, z, xh = lax.rem(dp, 2), lax.rem(lax.div(dp, 2), 8), lax.div(dp, 16)
    y, xl = lax.div(tn, 2), lax.rem(tn, 2)

    def device(h, k, c, t):
        return (h * 16 + k * 2 + c, t)

    def ring(value, size):
        return lax.rem(value + size, size)

    z_up = device(xh, ring(z + 1, 8), core, tn)
    z_dn = device(xh, ring(z - 1, 8), core, tn)
    x_far = device(1 - xh, z, core, tn)
    x_near = device(xh, z, core, y * 2 + 1 - xl)
    y_up = device(xh, z, core, ring(y + 1, 4) * 2 + xl)
    y_dn = device(xh, z, core, ring(y - 1, 4) * 2 + xl)
    other = device(xh, z, 1 - core, tn)

    def unit(h, k):
        return h * 8 + ring(k, 8)

    me = unit(xh, z)
    loads = [
        pltpu.make_async_copy(src, dst, load_sem.at[i])
        for i, (src, dst) in enumerate(((grad_hbm, grad_ref), (gate_hbm, gate_ref)))
    ]
    for load in loads:
        load.start()

    barrier = pltpu.get_barrier_semaphore()

    def greet(target):
        pl.semaphore_signal(barrier, inc=1, device_id=target, device_id_type=pl.DeviceIdType.MESH)

    def chip(t):
        return device(lax.div(t, 8), lax.rem(t, 8), core, tn)

    greet(other)
    for step in range(1, 8):
        greet(device(xh, z, core, ring(tn + step, 8)))
    for step in range(1, UNITS):
        greet(chip(ring(me + step, UNITS)))

    for load in loads:
        load.wait()
    up_grad = (
        grad_ref[...].astype(jnp.float32) * jax.nn.silu(gate_ref[...].astype(jnp.float32))
    ).astype(jnp.bfloat16)
    rows[me] = up_grad.T

    pl.semaphore_wait(barrier, 23)

    ROW, ROW_O, SCATTER, SPREAD, PLANE, PLANE_O = (sent.at[i] for i in range(6))

    def copy(src, dst, send, recv, target):
        return pltpu.make_async_remote_copy(
            src_ref=src, dst_ref=dst, send_sem=send, recv_sem=recv,
            device_id=target, device_id_type=pl.DeviceIdType.MESH,
        )

    def arrive(ref, recv):
        copy(ref, ref, sent.at[0], recv, other).wait_recv()

    def leave(ref, send):
        copy(ref, ref, send, load_sem.at[0], other).wait_send()

    def pass_on(kind, u, *targets, recv=None):
        ref = rows.at[u, SPAN[kind]]
        for target in targets:
            copy(ref, ref, ROW, row_recv.at[kind, u] if recv is None else recv, target).start()

    def share(kind, u, group):
        copy(
            rows.at[u, SPAN[kind]], rows_o.at[u, SPAN[kind]], ROW_O,
            rowo_recv.at[min(kind, B), group], other,
        ).start()

    def row_in(kind, u, group, *targets):
        arrive(rows.at[u, SPAN[kind]], row_recv.at[kind, u])
        pass_on(kind, u, *targets)
        share(kind, u, group)

    def half(h):
        return pl.ds(h * 8, 8)

    def piece(e, h, *targets):
        src = cols.at[e, half(h)]
        for target in targets:
            copy(src, src, PLANE, piece_recv.at[e, h], target).start()

        @pl.when(lax.div(e, 4) != core)
        def _():
            copy(src, cols_o.at[lax.rem(e, 4), half(h)], PLANE_O, colo_recv, other).start()

    def piece_in(e, h, *targets):
        arrive(cols.at[e, half(h)], piece_recv.at[e, h])
        piece(e, h, *targets)

    def part(m, e):
        return pl.ds(pl.multiple_of(m * 896 + e * PIECE, PIECE), PIECE)

    for step in range(1, 8):
        e = ring(tn + step, 8)
        for m in range(2):
            copy(
                rows.at[me, part(m, e)], stage.at[tn * 2 + m], SCATTER, stage_recv,
                device(xh, z, core, e),
            ).start()
    pass_on(A, me, z_up, z_dn)
    pass_on(B, me, x_far)
    pass_on(B, me, z_up, z_dn)
    pass_on(A, me, x_far)
    share(A, me, 0)
    share(B, me, 0)
    for m in range(2):
        stage[tn * 2 + m] = rows[me, part(m, tn), :]

    arrive(stage.at[pl.ds(0, 14)], stage_recv)
    for h, first in ((xh, 1), (1 - xh, 0)):
        for step in range(first, 8):
            t = unit(h, z + step)
            copy(stage.at[t], cols.at[tn, me], SPREAD, spread_recv.at[first], chip(t)).start()
    cols[tn, me] = stage[me]

    far, last, far_last = unit(1 - xh, z), unit(xh, z + 4), unit(1 - xh, z + 4)
    near_piece = y * 2 + 1 - xl
    dn, up, opp = ring(y - 1, 4) * 2, ring(y + 1, 4) * 2, ring(y + 2, 4) * 2

    def lo(j):
        return unit(xh, z - j)

    def hi(j):
        return unit(xh, z + j)

    def far_lo(j):
        return unit(1 - xh, z - j)

    def far_hi(j):
        return unit(1 - xh, z + j)

    def spread(h, first):
        arrive(stage.at[pl.ds(0, 8 - first)], spread_recv.at[first])
        piece(tn, h, x_near, y_up, y_dn)

    def hop(h):
        piece_in(dn + xl, h, y_up)
        piece_in(up + xl, h)
        piece_in(dn + 1 - xl, h)
        piece_in(up + 1 - xl, h, y_dn)

    def end(h):
        piece_in(opp + xl, h)
        piece_in(opp + 1 - xl, h)

    groups = [[me, far]] + [[lo(j), hi(j), far_lo(j), far_hi(j)] for j in range(1, 4)]
    groups = [groups[0] + groups[1], groups[2], groups[3], [last, far_last]]

    def multiply(kind, g):
        units = groups[g]
        arrive(rows_o.at[pl.ds(0, len(units)), SPAN[kind]], rowo_recv.at[kind, g])
        left = jnp.concatenate(
            [
                panel.reshape(COLS, TOK)
                for u in units
                for panel in (cols[pl.ds(core * 4, 4), u], cols_o[:, u])
            ],
            axis=1,
        )
        right = jnp.concatenate([r[u, PART[kind], :] for u in units for r in (rows, rows_o)], axis=1)
        total = lax.dot_general(left, right, NT, preferred_element_type=jnp.float32)
        if g > 0:
            total = total + out_ref[:, PART[kind]]
        if g == 3:
            total = total * (1.0 / 4096)
        out_ref[:, PART[kind]] = total

    row_in(A, lo(1), 0, z_up)
    row_in(A, hi(1), 0, z_dn)
    row_in(B, far, 0, z_up, z_dn)
    spread(xh, 1)
    spread(1 - xh, 0)
    pass_on(A, lo(1), x_far)
    pass_on(A, hi(1), x_far)
    piece_in(near_piece, xh, y_up, y_dn)
    row_in(A, lo(2), 1, z_up, x_far)
    row_in(A, hi(2), 1, z_dn, x_far)
    row_in(A, far, 0)
    row_in(B, hi(1), 0, z_dn)
    row_in(B, far_lo(1), 0, z_up)
    row_in(B, far_hi(1), 0, z_dn)
    piece_in(near_piece, 1 - xh, y_up, y_dn)
    row_in(A, lo(3), 2, z_up, x_far)
    row_in(A, hi(3), 2, x_far)
    row_in(B, lo(1), 0, z_up)
    hop(xh)
    row_in(B, hi(2), 1, z_dn)
    row_in(A, far_lo(1), 0)
    row_in(A, far_hi(1), 0)
    row_in(B, far_lo(2), 1, z_up)
    hop(1 - xh)
    row_in(B, far_hi(2), 1, z_dn)
    row_in(A, last, 3, x_far)
    end(xh)
    row_in(B, lo(2), 1, z_up)
    end(1 - xh)
    row_in(B, hi(3), 2, z_dn)
    arrive(cols_o, colo_recv)
    multiply(A, 0)
    row_in(A, far_lo(2), 1)
    row_in(A, far_hi(2), 1)
    multiply(B, 0)
    row_in(B, far_lo(3), 2)
    pass_on(C, far_lo(3), z_up, recv=split_recv.at[0])
    row_in(B, far_hi(3), 2)
    pass_on(D, far_hi(3), z_dn, recv=split_recv.at[1])
    multiply(A, 1)
    multiply(B, 1)
    row_in(A, far_lo(3), 2)
    row_in(A, far_hi(3), 2)
    row_in(B, lo(3), 2)
    row_in(B, last, 3)
    multiply(A, 2)
    row_in(A, far_last, 3)
    for kind in (C, D):
        arrive(rows.at[far_last, SPAN[kind]], split_recv.at[kind - C])
        share(kind, far_last, 3)
    multiply(B, 2)
    multiply(A, 3)
    multiply(B, 3)

    leave(rows.at[pl.ds(0, 15)], ROW)
    leave(rows, ROW_O)
    leave(stage.at[pl.ds(0, 14)], SCATTER)
    leave(stage.at[pl.ds(0, 15)], SPREAD)
    leave(cols.at[pl.ds(0, 7)], PLANE)
    leave(cols_o, PLANE_O)


def shards(grad_hidden, gate):
    dma = pltpu.SemaphoreType.DMA
    return pl.pallas_call(
        kernel,
        out_shape=jax.ShapeDtypeStruct((COLS, WIDTH), jnp.float32),
        in_specs=[pl.BlockSpec(memory_space=pltpu.HBM)] * 2,
        out_specs=pl.BlockSpec(memory_space=pltpu.VMEM),
        scratch_shapes=[
            pltpu.VMEM((TOK, WIDTH), jnp.bfloat16),
            pltpu.VMEM((TOK, WIDTH), jnp.bfloat16),
            pltpu.VMEM((UNITS, WIDTH, TOK), jnp.bfloat16),
            pltpu.VMEM((UNITS, WIDTH, TOK), jnp.bfloat16),
            pltpu.VMEM((8, UNITS, PIECE, TOK), jnp.bfloat16),
            pltpu.VMEM((4, UNITS, PIECE, TOK), jnp.bfloat16),
            pltpu.VMEM((UNITS, PIECE, TOK), jnp.bfloat16),
            dma((2, UNITS)),
            dma((2,)),
            dma((2, 4)),
            dma,
            dma((2,)),
            dma((8, 2)),
            dma,
            dma((6,)),
            dma((2,)),
        ],
        compiler_params=pltpu.CompilerParams(
            collective_id=0, has_side_effects=True, vmem_limit_bytes=40_000_000
        ),
    )(*(pltpu.with_memory_space_constraint(a, pltpu.HBM) for a in (grad_hidden, gate))).T


def solution(mesh):
    return jax.shard_map(
        shards,
        mesh=mesh,
        in_specs=(P("dp", "tensor"), P("dp", "tensor")),
        out_specs=P("tensor", "dp"),
        check_vma=False,
    )
```

```python
import jax
import jax.numpy as jnp
from jax import lax
from jax.experimental import pallas as pl
from jax.experimental.pallas import tpu as pltpu
from jax.sharding import PartitionSpec as P

WIDTH = 1792
TOK = 128
UNITS = 16
PIECE = 112
COLS = 448
A, B, C, D = range(4)
CUT, HALF = 864, 464
SPAN = (pl.ds(0, CUT), pl.ds(CUT, 2 * HALF), pl.ds(CUT, HALF), pl.ds(CUT + HALF, HALF))
PART = (pl.ds(0, 768), pl.ds(768, WIDTH - 768))
NT = (((1,), (1,)), ((), ()))


def kernel(
    grad_hbm, gate_hbm, out_ref, grad_ref, gate_ref, rows, rows_o, cols, cols_o, stage,
    row_recv, split_recv, rowo_recv, stage_recv, spread_recv, piece_recv, colo_recv, sent, load_sem,
):
    dp, tn = lax.axis_index("dp"), lax.axis_index("tensor")
    core, z, xh = lax.rem(dp, 2), lax.rem(lax.div(dp, 2), 8), lax.div(dp, 16)
    y, xl = lax.div(tn, 2), lax.rem(tn, 2)

    def device(h, k, c, t):
        return (h * 16 + k * 2 + c, t)

    def ring(value, size):
        return lax.rem(value + size, size)

    z_up = device(xh, ring(z + 1, 8), core, tn)
    z_dn = device(xh, ring(z - 1, 8), core, tn)
    x_far = device(1 - xh, z, core, tn)
    x_near = device(xh, z, core, y * 2 + 1 - xl)
    y_up = device(xh, z, core, ring(y + 1, 4) * 2 + xl)
    y_dn = device(xh, z, core, ring(y - 1, 4) * 2 + xl)
    other = device(xh, z, 1 - core, tn)

    def unit(h, k):
        return h * 8 + ring(k, 8)

    me = unit(xh, z)
    loads = [
        pltpu.make_async_copy(src, dst, load_sem.at[i])
        for i, (src, dst) in enumerate(((grad_hbm, grad_ref), (gate_hbm, gate_ref)))
    ]
    for load in loads:
        load.start()

    barrier = pltpu.get_barrier_semaphore()

    def greet(target):
        pl.semaphore_signal(barrier, inc=1, device_id=target, device_id_type=pl.DeviceIdType.MESH)

    def chip(t):
        return device(lax.div(t, 8), lax.rem(t, 8), core, tn)

    greet(other)
    for step in range(1, 8):
        greet(device(xh, z, core, ring(tn + step, 8)))
    for step in range(1, UNITS):
        greet(chip(ring(me + step, UNITS)))

    for load in loads:
        load.wait()
    up_grad = (
        grad_ref[...].astype(jnp.float32) * jax.nn.silu(gate_ref[...].astype(jnp.float32))
    ).astype(jnp.bfloat16)
    rows[me] = up_grad.T

    pl.semaphore_wait(barrier, 23)

    ROW, ROW_O, SCATTER, SPREAD, PLANE, PLANE_O = (sent.at[i] for i in range(6))

    def copy(src, dst, send, recv, target):
        return pltpu.make_async_remote_copy(
            src_ref=src, dst_ref=dst, send_sem=send, recv_sem=recv,
            device_id=target, device_id_type=pl.DeviceIdType.MESH,
        )

    def arrive(ref, recv):
        copy(ref, ref, sent.at[0], recv, other).wait_recv()

    def leave(ref, send):
        copy(ref, ref, send, load_sem.at[0], other).wait_send()

    def pass_on(kind, u, *targets, recv=None):
        ref = rows.at[u, SPAN[kind]]
        for target in targets:
            copy(ref, ref, ROW, row_recv.at[kind, u] if recv is None else recv, target).start()

    def share(kind, u, group):
        copy(
            rows.at[u, SPAN[kind]], rows_o.at[u, SPAN[kind]], ROW_O,
            rowo_recv.at[min(kind, B), group], other,
        ).start()

    def row_in(kind, u, group, *targets):
        arrive(rows.at[u, SPAN[kind]], row_recv.at[kind, u])
        pass_on(kind, u, *targets)
        share(kind, u, group)

    def half(h):
        return pl.ds(h * 8, 8)

    def piece(e, h, *targets):
        src = cols.at[e, half(h)]
        for target in targets:
            copy(src, src, PLANE, piece_recv.at[e, h], target).start()

        @pl.when(lax.div(e, 4) != core)
        def _():
            copy(src, cols_o.at[lax.rem(e, 4), half(h)], PLANE_O, colo_recv, other).start()

    def piece_in(e, h, *targets):
        arrive(cols.at[e, half(h)], piece_recv.at[e, h])
        piece(e, h, *targets)

    def part(m, e):
        return pl.ds(pl.multiple_of(m * 896 + e * PIECE, PIECE), PIECE)

    for step in range(1, 8):
        e = ring(tn + step, 8)
        for m in range(2):
            copy(
                rows.at[me, part(m, e)], stage.at[tn * 2 + m], SCATTER, stage_recv,
                device(xh, z, core, e),
            ).start()
    pass_on(A, me, z_up, z_dn)
    pass_on(B, me, x_far)
    pass_on(B, me, z_up, z_dn)
    pass_on(A, me, x_far)
    share(A, me, 0)
    share(B, me, 0)
    for m in range(2):
        stage[tn * 2 + m] = rows[me, part(m, tn), :]

    arrive(stage.at[pl.ds(0, 14)], stage_recv)
    for h, first in ((xh, 1), (1 - xh, 0)):
        for step in (4, 3, 5, 2, 6, 1, 7, 0)[: 8 - first]:
            t = unit(h, z + step)
            copy(stage.at[t], cols.at[tn, me], SPREAD, spread_recv.at[first], chip(t)).start()
    cols[tn, me] = stage[me]

    far, last, far_last = unit(1 - xh, z), unit(xh, z + 4), unit(1 - xh, z + 4)
    near_piece = y * 2 + 1 - xl
    dn, up, opp = ring(y - 1, 4) * 2, ring(y + 1, 4) * 2, ring(y + 2, 4) * 2

    def lo(j):
        return unit(xh, z - j)

    def hi(j):
        return unit(xh, z + j)

    def far_lo(j):
        return unit(1 - xh, z - j)

    def far_hi(j):
        return unit(1 - xh, z + j)

    def spread(h, first):
        arrive(stage.at[pl.ds(0, 8 - first)], spread_recv.at[first])
        piece(tn, h, x_near, y_up, y_dn)

    def hop(h):
        piece_in(dn + xl, h, y_up)
        piece_in(up + xl, h)
        piece_in(dn + 1 - xl, h)
        piece_in(up + 1 - xl, h, y_dn)

    def end(h):
        piece_in(opp + xl, h)
        piece_in(opp + 1 - xl, h)

    groups = [[me, far]] + [[lo(j), hi(j), far_lo(j), far_hi(j)] for j in range(1, 4)]
    groups = [groups[0] + groups[1], groups[2], groups[3], [last, far_last]]

    def multiply(kind, g):
        units = groups[g]
        arrive(rows_o.at[pl.ds(0, len(units)), SPAN[kind]], rowo_recv.at[kind, g])
        left = jnp.concatenate(
            [
                panel.reshape(COLS, TOK)
                for u in units
                for panel in (cols[pl.ds(core * 4, 4), u], cols_o[:, u])
            ],
            axis=1,
        )
        right = jnp.concatenate([r[u, PART[kind], :] for u in units for r in (rows, rows_o)], axis=1)
        total = lax.dot_general(left, right, NT, preferred_element_type=jnp.float32)
        if g > 0:
            total = total + out_ref[:, PART[kind]]
        if g == 3:
            total = total * (1.0 / 4096)
        out_ref[:, PART[kind]] = total

    row_in(A, lo(1), 0, z_up)
    row_in(A, hi(1), 0, z_dn)
    row_in(B, far, 0, z_up, z_dn)
    spread(xh, 1)
    spread(1 - xh, 0)
    pass_on(A, lo(1), x_far)
    pass_on(A, hi(1), x_far)
    piece_in(near_piece, xh, y_up, y_dn)
    row_in(A, lo(2), 1, z_up, x_far)
    row_in(A, hi(2), 1, z_dn, x_far)
    row_in(A, far, 0)
    row_in(B, hi(1), 0, z_dn)
    row_in(B, far_lo(1), 0, z_up)
    row_in(B, far_hi(1), 0, z_dn)
    piece_in(near_piece, 1 - xh, y_up, y_dn)
    row_in(A, lo(3), 2, z_up, x_far)
    row_in(A, hi(3), 2, x_far)
    row_in(B, lo(1), 0, z_up)
    hop(xh)
    row_in(B, hi(2), 1, z_dn)
    row_in(A, far_lo(1), 0)
    row_in(A, far_hi(1), 0)
    row_in(B, far_lo(2), 1, z_up)
    hop(1 - xh)
    row_in(B, far_hi(2), 1, z_dn)
    row_in(A, last, 3, x_far)
    end(xh)
    row_in(B, lo(2), 1, z_up)
    end(1 - xh)
    row_in(B, hi(3), 2, z_dn)
    arrive(cols_o, colo_recv)
    multiply(A, 0)
    row_in(A, far_lo(2), 1)
    row_in(A, far_hi(2), 1)
    multiply(B, 0)
    row_in(B, far_lo(3), 2)
    pass_on(C, far_lo(3), z_up, recv=split_recv.at[0])
    row_in(B, far_hi(3), 2)
    pass_on(D, far_hi(3), z_dn, recv=split_recv.at[1])
    multiply(A, 1)
    multiply(B, 1)
    row_in(A, far_lo(3), 2)
    row_in(A, far_hi(3), 2)
    row_in(B, lo(3), 2)
    row_in(B, last, 3)
    multiply(A, 2)
    row_in(A, far_last, 3)
    for kind in (C, D):
        arrive(rows.at[far_last, SPAN[kind]], split_recv.at[kind - C])
        share(kind, far_last, 3)
    multiply(B, 2)
    multiply(A, 3)
    multiply(B, 3)

    leave(rows.at[pl.ds(0, 15)], ROW)
    leave(rows, ROW_O)
    leave(stage.at[pl.ds(0, 14)], SCATTER)
    leave(stage.at[pl.ds(0, 15)], SPREAD)
    leave(cols.at[pl.ds(0, 7)], PLANE)
    leave(cols_o, PLANE_O)


def shards(grad_hidden, gate):
    dma = pltpu.SemaphoreType.DMA
    return pl.pallas_call(
        kernel,
        out_shape=jax.ShapeDtypeStruct((COLS, WIDTH), jnp.float32),
        in_specs=[pl.BlockSpec(memory_space=pltpu.HBM)] * 2,
        out_specs=pl.BlockSpec(memory_space=pltpu.VMEM),
        scratch_shapes=[
            pltpu.VMEM((TOK, WIDTH), jnp.bfloat16),
            pltpu.VMEM((TOK, WIDTH), jnp.bfloat16),
            pltpu.VMEM((UNITS, WIDTH, TOK), jnp.bfloat16),
            pltpu.VMEM((UNITS, WIDTH, TOK), jnp.bfloat16),
            pltpu.VMEM((8, UNITS, PIECE, TOK), jnp.bfloat16),
            pltpu.VMEM((4, UNITS, PIECE, TOK), jnp.bfloat16),
            pltpu.VMEM((UNITS, PIECE, TOK), jnp.bfloat16),
            dma((2, UNITS)),
            dma((2,)),
            dma((2, 4)),
            dma,
            dma((2,)),
            dma((8, 2)),
            dma,
            dma((6,)),
            dma((2,)),
        ],
        compiler_params=pltpu.CompilerParams(
            collective_id=0, has_side_effects=True, vmem_limit_bytes=40_000_000
        ),
    )(*(pltpu.with_memory_space_constraint(a, pltpu.HBM) for a in (grad_hidden, gate))).T


def solution(mesh):
    return jax.shard_map(
        shards,
        mesh=mesh,
        in_specs=(P("dp", "tensor"), P("dp", "tensor")),
        out_specs=P("tensor", "dp"),
        check_vma=False,
    )
```
